32 devices in a mesh: band: 16 (over z, y, core), ga: 2 (over x).
Axes of the slice: x: 2, y: 2, z: 4, core: 2. Of those that a mesh axis runs over, the one named last changes fastest.
Arguments:
- orbitals: bfloat16 [2, 16, 160, 128], P(None, 'band', 'ga'), may hold values from -8 to 8, as said below
- potential: float32 [480, 480], P('ga'), may hold values from -2 to 2
- slot_sticks: int32 [160], replicated, may hold values from -1 to 126, as said below
- stick_entries: int32 [160, 128], replicated, may hold values from -1 to 126, as said below
Outputs:
- applied_orbitals: bfloat16 [2, 16, 160, 128], P(None, 'band', 'ga')
- correlation: float32 [2, 16, 16], replicated
- reduced_hamiltonian: float32 [2, 16, 16], replicated
The draws below stay inside these ranges and needn't reach their ends.
Inputs may be any that keep to these rules, and one draw needn't show every extreme that they name: `slot_sticks`: every gx with |gx| < 64 is held by exactly one slot; the other slots hold -1. Slots t with t // 80 = d are those of index d of ga; on some index of ga all 80 slots hold sticks. `stick_entries`: row t lists, in some order, gz + 63 for every gz with gx^2 + gz^2 < 64^2, gx being the stick of slot t, then -1 to the end of the row; rows of empty slots are all -1. `orbitals`: entries where stick_entries is -1 carry values that are not used.
All inputs are finite; a program needn't handle non-finite values.
Results may differ from the reference program's by a relative error of at most 0.001.
Values may be sent and summed in bfloat16 or wider, within the bound.
A program may use at most 64 MiB of HBM per device.

```python
import jax
import jax.numpy as jnp
from jax import lax

NGRID = 480
RAD = 64
KMAX = 128
SLOTS = 80
SLOT_ALL = 160
NB = 16
N_GA = 2


def stick_layout(key):
    stick_count = 2 * RAD - 1
    key_device, key_picked, key_ordering = jax.random.split(jax.random.fold_in(key, 11), 3)
    full_device = jax.random.randint(key_device, (), 0, N_GA)
    slot_ids = jnp.arange(SLOT_ALL, dtype=jnp.int32)
    owners = slot_ids // SLOTS
    others = jnp.where(owners > full_device, slot_ids - SLOTS, slot_ids)
    picked = jax.random.permutation(key_picked, (N_GA - 1) * SLOTS).astype(jnp.int32)
    chosen = jnp.take(picked, jnp.clip(others, 0, (N_GA - 1) * SLOTS - 1)) < stick_count - SLOTS
    occupied = jnp.where(owners == full_device, True, chosen)
    ranking = jnp.cumsum(occupied.astype(jnp.int32)) - 1
    ordering = jax.random.permutation(key_ordering, stick_count).astype(jnp.int32)
    return jnp.where(occupied, jnp.take(ordering, jnp.clip(ranking, 0, stick_count - 1)), -1).astype(jnp.int32)


def draw_slot_sticks(key, part):
    return stick_layout(key)


def draw_stick_entries(key, part):
    sticks = stick_layout(key)
    gx_value = sticks - RAD + 1
    offsets = jnp.arange(RAD, dtype=jnp.int32)
    half_width = jnp.sum((offsets * offsets)[None, :] + (gx_value * gx_value)[:, None] < RAD * RAD, axis=1).astype(jnp.int32) - 1
    length = jnp.where(sticks >= 0, 2 * half_width + 1, 0)
    column_ids = jnp.arange(KMAX, dtype=jnp.int32)
    inside = column_ids[None, :] < length[:, None]
    positions = jnp.where(inside, RAD - 1 - half_width[:, None] + column_ids[None, :], -1)
    jitter = jax.random.randint(jax.random.fold_in(key, 23), (SLOT_ALL, KMAX), 0, 4096)
    scores = jnp.where(inside, jitter, 4096) * KMAX + column_ids[None, :]
    ordering = jnp.argsort(scores, axis=1)
    return jnp.take_along_axis(positions, ordering, axis=1).astype(jnp.int32)


def draw_orbitals(key, part):
    key_own, key_common, key_weight, key_flip = jax.random.split(jax.random.fold_in(key, 37), 4)
    private = jax.random.normal(key_own, (2, NB, SLOT_ALL, KMAX), jnp.float32)
    weight = jax.random.uniform(key_weight, (NB,), jnp.float32, 0.5, 1.5)
    common = jax.random.normal(key_common, (2, 1, SLOT_ALL, KMAX), jnp.float32)
    sign_flip = jnp.where(jax.random.bernoulli(key_flip, 0.5, (NB,)), 1.0, -1.0)
    values = private + (weight * sign_flip)[None, :, None, None] * common
    return jnp.clip(values, -8.0, 8.0).astype(jnp.bfloat16)


def steps_of(rng, shape, pieces, smallest, high):
    loudness, own = 1.0, jax.random.fold_in(rng, 6)
    for dim, parts in pieces:
        steps = jnp.exp(jax.random.uniform(jax.random.fold_in(own, dim), (parts,), jnp.float32, smallest / len(pieces), high / len(pieces)))
        loudness = loudness * jnp.repeat(steps, shape[dim] // parts).reshape([-1 if axis == dim else 1 for axis in range(len(shape))])
    return loudness


def setup_inputs(seed: int = 0) -> dict:
    key_of = jax.random.split(jax.random.key(seed), 5)
    return {
        "orbitals": draw_orbitals(jax.random.fold_in(key_of[4], 71), 0),
        "potential": jnp.clip(jax.random.uniform(key_of[1], (NGRID, NGRID), jnp.float32, -2.0, 2.0) * steps_of(key_of[1], (NGRID, NGRID), ((0, 2),), -0.4, 0.0), -2.0, 2.0),
        "slot_sticks": draw_slot_sticks(jax.random.fold_in(key_of[4], 71), 0),
        "stick_entries": draw_stick_entries(jax.random.fold_in(key_of[4], 71), 0),
    }


TWO_PI = 6.283185307179586
HIGHEST_PRECISION = lax.Precision.HIGHEST


def phases(frequency, position, points):
    winding = (frequency[:, None] * position[None, :]) % points
    angles = winding.astype(jnp.float32) * (TWO_PI / points)
    return jnp.cos(angles), jnp.sin(angles)


def stick_phases(slot_sticks, radius, points):
    frequency = slot_sticks - radius + 1
    x_cos, x_sin = phases(frequency, jnp.arange(points, dtype=jnp.int32), points)
    filled = (slot_sticks >= 0).astype(jnp.float32)[:, None]
    return x_cos * filled, x_sin * filled


def unpack(coeffs, entry_lists):
    slot_count, width = entry_lists.shape
    leading = coeffs.shape[:2]
    flat_index = jnp.where(entry_lists >= 0, entry_lists + width * jnp.arange(slot_count, dtype=jnp.int32)[:, None], slot_count * width)
    spread = jnp.zeros(leading + (slot_count * width,), jnp.float32)
    values = coeffs.reshape(leading + (slot_count * width,)).astype(jnp.float32)
    spread = spread.at[:, :, flat_index.reshape(-1)].add(values, mode="drop")
    return spread.reshape(coeffs.shape)


def z_forward(spread, z_cos, z_sin):
    real_part = jnp.einsum("bsp,pz->bsz", spread[0], z_cos, precision=HIGHEST_PRECISION) - jnp.einsum("bsp,pz->bsz", spread[1], z_sin, precision=HIGHEST_PRECISION)
    imag_part = jnp.einsum("bsp,pz->bsz", spread[0], z_sin, precision=HIGHEST_PRECISION) + jnp.einsum("bsp,pz->bsz", spread[1], z_cos, precision=HIGHEST_PRECISION)
    return jnp.stack([real_part, imag_part])


def plane_work(columns, x_cos, x_sin, potential):
    field_real = jnp.einsum("bsz,sx->bzx", columns[0], x_cos, precision=HIGHEST_PRECISION) - jnp.einsum("bsz,sx->bzx", columns[1], x_sin, precision=HIGHEST_PRECISION)
    field_imag = jnp.einsum("bsz,sx->bzx", columns[0], x_sin, precision=HIGHEST_PRECISION) + jnp.einsum("bsz,sx->bzx", columns[1], x_cos, precision=HIGHEST_PRECISION)
    prod_real = potential[None] * field_real
    prod_imag = potential[None] * field_imag
    back_real = jnp.einsum("bzx,sx->bsz", prod_real, x_cos, precision=HIGHEST_PRECISION) + jnp.einsum("bzx,sx->bsz", prod_imag, x_sin, precision=HIGHEST_PRECISION)
    back_imag = jnp.einsum("bzx,sx->bsz", prod_imag, x_cos, precision=HIGHEST_PRECISION) - jnp.einsum("bzx,sx->bsz", prod_real, x_sin, precision=HIGHEST_PRECISION)
    return jnp.stack([back_real, back_imag])


def z_backward(gathered, z_cos, z_sin, points):
    real_part = jnp.einsum("bsz,pz->bsp", gathered[0], z_cos, precision=HIGHEST_PRECISION) + jnp.einsum("bsz,pz->bsp", gathered[1], z_sin, precision=HIGHEST_PRECISION)
    imag_part = jnp.einsum("bsz,pz->bsp", gathered[1], z_cos, precision=HIGHEST_PRECISION) - jnp.einsum("bsz,pz->bsp", gathered[0], z_sin, precision=HIGHEST_PRECISION)
    return jnp.stack([real_part, imag_part]) / float(points * points)


def kinetic_factor(sticks, entry_lists, radius):
    gx_value = sticks - radius + 1
    gz_value = entry_lists - radius + 1
    return ((gx_value * gx_value)[:, None] + gz_value * gz_value).astype(jnp.float32) / float(radius * radius)


def cross_products(left, right, scale):
    dims = (((1,), (1,)), ((), ()))
    real_part = lax.dot_general(left[0], right[0], dims, preferred_element_type=jnp.float32) + lax.dot_general(left[1], right[1], dims, preferred_element_type=jnp.float32)
    imag_part = lax.dot_general(left[0], right[1], dims, preferred_element_type=jnp.float32) - lax.dot_general(left[1], right[0], dims, preferred_element_type=jnp.float32)
    return jnp.stack([real_part, imag_part]) * scale


def reference(orbitals, potential, slot_sticks, stick_entries):
    points = potential.shape[1]
    width = stick_entries.shape[1]
    radius = width // 2
    band_total = orbitals.shape[1]
    present = stick_entries >= 0
    masked = jnp.where(present[None, None], orbitals, jnp.zeros_like(orbitals))
    spread = unpack(orbitals, stick_entries)
    frequency = jnp.arange(width, dtype=jnp.int32) - radius + 1
    z_cos, z_sin = phases(frequency, jnp.arange(points, dtype=jnp.int32), points)
    x_cos, x_sin = stick_phases(slot_sticks, radius, points)

    def one_band(coeffs):
        columns = z_forward(coeffs[:, None], z_cos, z_sin)
        gathered = plane_work(columns, x_cos, x_sin, potential)
        return z_backward(gathered, z_cos, z_sin, points)[:, 0]

    spectra = jnp.moveaxis(lax.map(one_band, jnp.moveaxis(spread, 1, 0)), 0, 1)
    indices = jnp.broadcast_to(jnp.clip(stick_entries, 0, width - 1)[None, None], spectra.shape)
    applied = jnp.take_along_axis(spectra, indices, axis=3)
    kinetic = kinetic_factor(slot_sticks, stick_entries, radius)
    applied_orbitals = jnp.where(present[None, None], kinetic[None, None] * orbitals.astype(jnp.float32) + applied, jnp.float32(0.0)).astype(jnp.bfloat16)
    scale = 1.0 / (4.0 * radius * radius)
    flat_psi = masked.reshape(2, band_total, -1)
    flat_h = applied_orbitals.reshape(2, band_total, -1)
    correlation = cross_products(flat_psi, flat_psi, scale)
    reduced_hamiltonian = cross_products(flat_psi, flat_h, scale)
    return applied_orbitals, correlation, reduced_hamiltonian
```

```python
import functools

import jax
import jax.numpy as jnp
import numpy as np
from jax import lax
from jax.experimental import pallas as pl
from jax.experimental.pallas import tpu as pltpu
from jax.sharding import PartitionSpec as P

MESH = pl.DeviceIdType.MESH
NT = (((1,), (1,)), ((), ()))
BF16 = jnp.bfloat16
F32 = jnp.float32


def split_np(table):
    high = table.astype(np.float32).astype(BF16)
    low = (table - high.astype(np.float64)).astype(np.float32).astype(BF16)
    return np.stack([high, low])


def tables(points, width, radius, groups, planes, plane_pad, coarse):
    freq = np.arange(width) - radius + 1
    used = (np.arange(width) < width - 1).astype(np.float64)
    z_tabs = []
    for group in range(groups):
        z = np.arange(planes) + group * planes
        angle = 2.0 * np.pi * ((freq[:, None] * z[None, :]) % points) / points
        cos = np.zeros((width, plane_pad))
        sin = np.zeros((width, plane_pad))
        cos[:, :planes] = np.cos(angle) * used[:, None]
        sin[:, :planes] = np.sin(angle) * used[:, None]
        z_tabs.append(split_np(np.block([[cos, sin], [-sin, cos]])))
    x = np.arange(coarse)
    angle = 2.0 * np.pi * ((freq[None, :] * x[:, None]) % coarse) / coarse
    cos = np.cos(angle) * used[None, :]
    sin = np.sin(angle) * used[None, :]
    forward = np.block([[cos, -sin], [sin, cos]])
    limit = 2 * (radius - 1)
    offset = (x[:, None] * points - np.arange(points)[None, :] * coarse) % (coarse * points)
    base = 2.0 * np.pi * offset / (coarse * points)
    resample = np.ones((coarse, points))
    for g in range(1, limit + 1):
        resample += 2.0 * np.cos(g * base)
    resample /= points
    return (
        np.stack(z_tabs),
        split_np(forward),
        split_np(forward.T.copy()),
        split_np(resample),
    )


def split(value):
    high = value.astype(BF16)
    low = (value - high.astype(F32)).astype(BF16)
    return high, low


def dot(a, b):
    return jnp.dot(a, b, preferred_element_type=F32)


def dot_nt(a, b):
    return lax.dot_general(a, b, NT, preferred_element_type=F32)


def take_lanes(value, index):
    return jnp.take_along_axis(value, index, axis=1, mode="promise_in_bounds")


def kernel(
    bands,
    groups,
    points,
    radius,
    orb_ref,
    slots_ref,
    entries_ref,
    pot_hbm,
    tz_hbm,
    tx_hbm,
    ty_hbm,
    tr_hbm,
    out_ref,
    corr_ref,
    red_ref,
    tz,
    tx,
    ty,
    tr,
    pot,
    spread,
    colbuf,
    part,
    got,
    gather,
    sums,
    message,
    inbox,
    load_sem,
    s_send,
    s_recv,
    p_send,
    p_recv,
    g_send,
    g_recv,
    m_send,
    m_recv,
):
    band = lax.axis_index("band")
    ga = lax.axis_index("ga")
    total = bands * groups
    me = ga * bands + band
    slots = orb_ref.shape[2]
    width = orb_ref.shape[3]
    planes = pot_hbm.shape[0]
    plane_pad = pot.shape[0]
    coarse = ty.shape[2] // 2
    msg_width = message.shape[1]

    def where_is(index):
        return (lax.rem(index, bands), lax.div(index, bands))

    barrier = pltpu.get_barrier_semaphore()

    @pl.loop(1, total)
    def _(k):
        pl.semaphore_signal(
            barrier, inc=1, device_id=where_is(lax.rem(me + k, total)), device_id_type=MESH
        )

    loads = [
        pltpu.make_async_copy(pot_hbm, pot.at[pl.ds(0, planes)], load_sem.at[0]),
        pltpu.make_async_copy(tr_hbm, tr, load_sem.at[1]),
        pltpu.make_async_copy(tz_hbm.at[ga], tz, load_sem.at[2]),
        pltpu.make_async_copy(tx_hbm, tx, load_sem.at[3]),
        pltpu.make_async_copy(ty_hbm, ty, load_sem.at[4]),
    ]
    for load in loads:
        load.start()
    if plane_pad > planes:
        pot[pl.ds(planes, plane_pad - planes), :] = jnp.zeros(
            (plane_pad - planes, pot.shape[1]), F32
        )

    sums[...] = jnp.zeros_like(sums)

    own = entries_ref[pl.ds(pl.multiple_of(ga * slots, 8), slots), :]
    lane = lax.broadcasted_iota(jnp.int32, (slots, width), 1)
    inverse = jnp.full((slots, width), -1, jnp.int32)
    for k in range(width):
        inverse = jnp.where(own[:, k : k + 1] == lane, k, inverse)
    re = orb_ref[0, 0].astype(F32)
    im = orb_ref[1, 0].astype(F32)
    filled = inverse >= 0
    index = jnp.maximum(inverse, 0)
    spread[ga, :, :width] = jnp.where(filled, take_lanes(re, index), 0.0).astype(BF16)
    spread[ga, :, width:] = jnp.where(filled, take_lanes(im, index), 0.0).astype(BF16)

    pl.semaphore_wait(barrier, total - 1)

    s_copies = []
    for k in range(1, groups):
        copy = pltpu.make_async_remote_copy(
            src_ref=spread.at[ga],
            dst_ref=spread.at[ga],
            send_sem=s_send.at[k - 1],
            recv_sem=s_recv.at[k - 1],
            device_id=(band, lax.rem(ga + k, groups)),
            device_id_type=MESH,
        )
        copy.start()
        s_copies.append(copy)

    def gather_copy(k):
        return pltpu.make_async_remote_copy(
            src_ref=orb_ref.at[:, 0],
            dst_ref=gather.at[band],
            send_sem=g_send.at[k],
            recv_sem=g_recv.at[k],
            device_id=(lax.rem(band + k, bands), ga),
            device_id_type=MESH,
        )

    @pl.loop(1, bands)
    def _(k):
        gather_copy(k).start()

    loads[0].wait()
    loads[1].wait()
    pot_hi, pot_lo = split(pot[...])
    weight = dot_nt(tr[0], pot_hi) + dot_nt(tr[0], pot_lo) + dot_nt(tr[1], pot_hi)

    for copy in s_copies:
        copy.wait()
    dense = jnp.zeros((width, 2 * width), F32)
    sub = lax.broadcasted_iota(jnp.int32, (width, slots), 0)
    for g in range(groups):
        choose = jnp.where(sub == slots_ref[g : g + 1, :], 1.0, 0.0).astype(BF16)
        dense += dot(choose, spread[g])
    dense = dense.astype(BF16)

    loads[2].wait()
    columns = dot(dense, tz[0]) + dot(dense, tz[1])
    col_hi, col_lo = split(columns)
    colbuf[0, :width] = col_hi[:, :plane_pad]
    colbuf[0, width:] = col_hi[:, plane_pad:]
    colbuf[1, :width] = col_lo[:, :plane_pad]
    colbuf[1, width:] = col_lo[:, plane_pad:]
    loads[3].wait()
    field = dot(tx[0], colbuf[0]) + dot(tx[0], colbuf[1]) + dot(tx[1], colbuf[0])
    product = jnp.concatenate([field[:coarse] * weight, field[coarse:] * weight], axis=0)
    pro_hi, pro_lo = split(product)
    loads[4].wait()
    back = dot(ty[0], pro_hi) + dot(ty[0], pro_lo) + dot(ty[1], pro_hi)
    back = jnp.concatenate([back[:width], back[width:]], axis=1)
    back_hi, back_lo = split(back)
    spectra = dot_nt(back_hi, tz[0]) + dot_nt(back_hi, tz[1]) + dot_nt(back_lo, tz[0])
    spectra = spectra * (1.0 / float(points * coarse))
    spec_hi, spec_lo = split(spectra)

    eye = lax.broadcasted_iota(jnp.int32, (slots, slots), 0) == lax.broadcasted_iota(
        jnp.int32, (slots, slots), 1
    )

    def stick_column(g):
        row = slots_ref[pl.ds(g, 1), :].astype(F32)
        return jnp.sum(jnp.where(eye, row, 0.0), axis=1, keepdims=True)

    lane_f = lane.astype(F32)
    p_copies = []
    for k in range(1, groups + 1):
        target = lax.rem(ga + k, groups)
        stick = stick_column(target)
        choose = jnp.where(stick == lane_f, 1.0, 0.0).astype(BF16)
        mine = dot(choose, spec_hi) + dot(choose, spec_lo)
        if k < groups:
            part[k - 1] = mine
            copy = pltpu.make_async_remote_copy(
                src_ref=part.at[k - 1],
                dst_ref=got.at[k - 1],
                send_sem=p_send.at[k - 1],
                recv_sem=p_recv.at[k - 1],
                device_id=(band, target),
                device_id_type=MESH,
            )
            copy.start()
            p_copies.append(copy)

    present = own >= 0
    gx = stick - float(radius - 1)
    gz = (own - (radius - 1)).astype(F32)
    kinetic = (gx * gx + gz * gz) * (1.0 / float(radius * radius))
    own_index = jnp.maximum(own, 0)

    gather[band] = orb_ref[:, 0]

    @pl.loop(1, bands)
    def _(k):
        gather_copy(k).wait()

    m_re = jnp.where(present, re, 0.0)
    m_im = jnp.where(present, im, 0.0)

    def add_products(first, right_re, right_im):
        @pl.loop(0, bands)
        def _(b):
            left_re = gather[b, 0].astype(F32)
            left_im = gather[b, 1].astype(F32)
            real = left_re * right_re + left_im * right_im
            imag = left_re * right_im - left_im * right_re
            sums[pl.ds(first * bands + b, 1), :] = jnp.sum(real, axis=0, keepdims=True)
            sums[pl.ds((first + 1) * bands + b, 1), :] = jnp.sum(imag, axis=0, keepdims=True)

    add_products(0, m_re, m_im)

    for copy in p_copies:
        copy.wait()
    for k in range(1, groups):
        mine += got[k - 1]
    a_re = take_lanes(mine[:, :width], own_index)
    a_im = take_lanes(mine[:, width:], own_index)
    h_re = jnp.where(present, kinetic * re + a_re, 0.0).astype(BF16)
    h_im = jnp.where(present, kinetic * im + a_im, 0.0).astype(BF16)
    out_ref[0, 0] = h_re
    out_ref[1, 0] = h_im
    add_products(2, h_re.astype(F32), h_im.astype(F32))

    ones = jnp.full((8, width), 1.0 / float(4 * radius * radius), F32)
    row = lax.dot_general(
        ones, sums[...], NT, preferred_element_type=F32, precision=lax.Precision.HIGHEST
    )
    message[...] = row[:1]
    inbox[pl.ds(me, 1), 0, :] = row[:1]

    @pl.loop(1, total)
    def _(k):
        pltpu.make_async_remote_copy(
            src_ref=message,
            dst_ref=inbox.at[me],
            send_sem=m_send,
            recv_sem=m_recv,
            device_id=where_is(lax.rem(me + k, total)),
            device_id_type=MESH,
        ).start()

    everyone = inbox.at[pl.ds(0, total - 1)]
    pltpu.make_async_copy(everyone, everyone, m_recv).wait()
    pltpu.make_async_copy(everyone, everyone, m_send).wait()

    rows = inbox[0:bands, 0, :]
    for g in range(1, groups):
        rows += inbox[g * bands : (g + 1) * bands, 0, :]
    unit = (
        lax.broadcasted_iota(jnp.int32, (msg_width, msg_width), 0)
        == lax.broadcasted_iota(jnp.int32, (msg_width, msg_width), 1)
    ).astype(F32)
    turned = lax.dot_general(
        unit, rows, NT, preferred_element_type=F32, precision=lax.Precision.HIGHEST
    )
    for c in range(2):
        corr_ref[c] = turned[c * bands : (c + 1) * bands]
        red_ref[c] = turned[(c + 2) * bands : (c + 3) * bands]


def body(bands, groups, orbitals, potential, slot_sticks, stick_entries):
    points = potential.shape[1]
    planes = potential.shape[0]
    width = stick_entries.shape[1]
    radius = width // 2
    slots = orbitals.shape[2]
    plane_pad = -(-planes // 128) * 128
    coarse = 2 * width
    sum_rows = -(-4 * bands // 128) * 128
    tz, tx, ty, tr = tables(points, width, radius, groups, planes, plane_pad, coarse)
    vmem = pl.BlockSpec(memory_space=pltpu.VMEM)
    hbm = pl.BlockSpec(memory_space=pl.ANY)
    total = bands * groups
    dma = pltpu.SemaphoreType.DMA
    return pl.pallas_call(
        functools.partial(kernel, bands, groups, points, radius),
        out_shape=(
            jax.ShapeDtypeStruct(orbitals.shape, BF16),
            jax.ShapeDtypeStruct((2, bands, bands), F32),
            jax.ShapeDtypeStruct((2, bands, bands), F32),
        ),
        in_specs=[vmem, vmem, vmem, hbm, hbm, hbm, hbm, hbm],
        out_specs=(vmem, vmem, vmem),
        scratch_shapes=[
            pltpu.VMEM(tz.shape[1:], BF16),
            pltpu.VMEM(tx.shape, BF16),
            pltpu.VMEM(ty.shape, BF16),
            pltpu.VMEM(tr.shape, BF16),
            pltpu.VMEM((plane_pad, points), F32),
            pltpu.VMEM((groups, slots, 2 * width), BF16),
            pltpu.VMEM((2, 2 * width, plane_pad), BF16),
            pltpu.VMEM((groups - 1, slots, 2 * width), F32),
            pltpu.VMEM((groups - 1, slots, 2 * width), F32),
            pltpu.VMEM((bands, 2, slots, width), BF16),
            pltpu.VMEM((sum_rows, width), F32),
            pltpu.VMEM((1, sum_rows), F32),
            pltpu.VMEM((total, 1, sum_rows), F32),
            dma((5,)),
            dma((groups - 1,)),
            dma((groups - 1,)),
            dma((groups - 1,)),
            dma((groups - 1,)),
            dma((bands,)),
            dma((bands,)),
            dma,
            dma,
        ],
        compiler_params=pltpu.CompilerParams(
            collective_id=0, has_side_effects=True, vmem_limit_bytes=48 * 1024 * 1024
        ),
    )(orbitals, slot_sticks.reshape(groups, slots), stick_entries, potential, tz, tx, ty, tr)


def solution(mesh):
    bands = mesh.shape["band"]
    groups = mesh.shape["ga"]
    return jax.shard_map(
        functools.partial(body, bands, groups),
        mesh=mesh,
        in_specs=(P(None, "band", "ga", None), P("ga", None), P(), P()),
        out_specs=(P(None, "band", "ga", None), P(), P()),
        check_vma=False,
    )
```

```python
import functools

import jax
import jax.numpy as jnp
import numpy as np
from jax import lax
from jax.experimental import pallas as pl
from jax.experimental.pallas import tpu as pltpu
from jax.sharding import PartitionSpec as P

MESH = pl.DeviceIdType.MESH
NT = (((1,), (1,)), ((), ()))
BF16 = jnp.bfloat16
F32 = jnp.float32


def split_np(table):
    high = table.astype(np.float32).astype(BF16)
    low = (table - high.astype(np.float64)).astype(np.float32).astype(BF16)
    return np.stack([high, low])


def tables(points, width, radius, groups, planes, plane_pad, coarse):
    freq = np.arange(width) - radius + 1
    used = (np.arange(width) < width - 1).astype(np.float64)
    z_tabs = []
    for group in range(groups):
        z = np.arange(planes) + group * planes
        angle = 2.0 * np.pi * ((freq[:, None] * z[None, :]) % points) / points
        cos = np.zeros((width, plane_pad))
        sin = np.zeros((width, plane_pad))
        cos[:, :planes] = np.cos(angle) * used[:, None]
        sin[:, :planes] = np.sin(angle) * used[:, None]
        z_tabs.append(split_np(np.block([[cos, sin], [-sin, cos]])))
    x = np.arange(coarse)
    angle = 2.0 * np.pi * ((freq[None, :] * x[:, None]) % coarse) / coarse
    cos = np.cos(angle) * used[None, :]
    sin = np.sin(angle) * used[None, :]
    forward = np.block([[cos, -sin], [sin, cos]])
    limit = 2 * (radius - 1)
    offset = (x[:, None] * points - np.arange(points)[None, :] * coarse) % (coarse * points)
    base = 2.0 * np.pi * offset / (coarse * points)
    resample = np.ones((coarse, points))
    for g in range(1, limit + 1):
        resample += 2.0 * np.cos(g * base)
    resample /= points
    return (
        np.stack(z_tabs),
        split_np(forward),
        split_np(forward.T.copy()),
        split_np(resample),
    )


def split(value):
    high = value.astype(BF16)
    low = (value - high.astype(F32)).astype(BF16)
    return high, low


def dot(a, b):
    return jnp.dot(a, b, preferred_element_type=F32)


def dot_nt(a, b):
    return lax.dot_general(a, b, NT, preferred_element_type=F32)


def take_lanes(value, index):
    return jnp.take_along_axis(value, index, axis=1, mode="promise_in_bounds")


def kernel(
    bands,
    groups,
    points,
    radius,
    orb_hbm,
    slots_hbm,
    entries_hbm,
    pot_hbm,
    tz_hbm,
    tx_hbm,
    ty_hbm,
    tr_hbm,
    out_ref,
    corr_ref,
    red_ref,
    orb_ref,
    slots_ref,
    entries_ref,
    tz,
    tx,
    ty,
    tr,
    pot,
    spread,
    colbuf,
    part,
    got,
    gather,
    sums,
    message,
    inbox,
    load_sem,
    s_send,
    s_recv,
    p_send,
    p_recv,
    g_send,
    g_recv,
    m_send,
    m_recv,
):
    band = lax.axis_index("band")
    ga = lax.axis_index("ga")
    total = bands * groups
    half = bands // 2
    me = ga * bands + band
    slots = orb_hbm.shape[2]
    width = orb_hbm.shape[3]
    planes = pot_hbm.shape[0]
    plane_pad = pot.shape[0]
    coarse = ty.shape[2] // 2
    msg_width = message.shape[1]

    def where_is(index):
        return (lax.rem(index, bands), lax.div(index, bands))

    barrier = pltpu.get_barrier_semaphore()

    @pl.loop(1, total)
    def _(k):
        pl.semaphore_signal(
            barrier, inc=1, device_id=where_is(lax.rem(me + k, total)), device_id_type=MESH
        )

    first = [
        pltpu.make_async_copy(
            entries_hbm.at[pl.ds(pl.multiple_of(ga * slots, 8), slots)], entries_ref, load_sem.at[5]
        ),
        pltpu.make_async_copy(orb_hbm, orb_ref, load_sem.at[6]),
        pltpu.make_async_copy(slots_hbm, slots_ref, load_sem.at[7]),
    ]
    for load in first:
        load.start()
    loads = [
        pltpu.make_async_copy(pot_hbm, pot.at[pl.ds(0, planes)], load_sem.at[0]),
        pltpu.make_async_copy(tr_hbm, tr, load_sem.at[1]),
        pltpu.make_async_copy(tz_hbm.at[ga], tz, load_sem.at[2]),
        pltpu.make_async_copy(tx_hbm, tx, load_sem.at[3]),
        pltpu.make_async_copy(ty_hbm, ty, load_sem.at[4]),
    ]
    for load in loads:
        load.start()
    if plane_pad > planes:
        pot[pl.ds(planes, plane_pad - planes), :] = jnp.zeros(
            (plane_pad - planes, pot.shape[1]), F32
        )

    sums[...] = jnp.zeros_like(sums)

    for load in first:
        load.wait()
    own = entries_ref[...]
    all_sticks = slots_ref[...].reshape(1, groups * slots)
    sticks = [all_sticks[:, g * slots : (g + 1) * slots] for g in range(groups)]
    lane = lax.broadcasted_iota(jnp.int32, (slots, width), 1)
    inverse = jnp.full((slots, width), -1, jnp.int32)
    for k in range(width):
        inverse = jnp.where(own[:, k : k + 1] == lane, k, inverse)
    re = orb_ref[0, 0].astype(F32)
    im = orb_ref[1, 0].astype(F32)
    filled = inverse >= 0
    index = jnp.maximum(inverse, 0)
    spread[ga, :, :width] = jnp.where(filled, take_lanes(re, index), 0.0).astype(BF16)
    spread[ga, :, width:] = jnp.where(filled, take_lanes(im, index), 0.0).astype(BF16)

    pl.semaphore_wait(barrier, total - 1)

    s_copies = []
    for k in range(1, groups):
        copy = pltpu.make_async_remote_copy(
            src_ref=spread.at[ga],
            dst_ref=spread.at[ga],
            send_sem=s_send.at[k - 1],
            recv_sem=s_recv.at[k - 1],
            device_id=(band, lax.rem(ga + k, groups)),
            device_id_type=MESH,
        )
        copy.start()
        s_copies.append(copy)

    def gather_copy(k):
        return pltpu.make_async_remote_copy(
            src_ref=orb_hbm.at[:, 0],
            dst_ref=gather.at[k],
            send_sem=g_send.at[k],
            recv_sem=g_recv.at[k],
            device_id=(lax.rem(band + k, bands), ga),
            device_id_type=MESH,
        )

    @pl.loop(1, half + 1)
    def _(k):
        gather_copy(k).start()

    loads[0].wait()
    loads[1].wait()
    pot_hi, pot_lo = split(pot[...])
    weight = dot_nt(tr[0], pot_hi) + dot_nt(tr[0], pot_lo) + dot_nt(tr[1], pot_hi)

    for copy in s_copies:
        copy.wait()
    dense = jnp.zeros((width, 2 * width), F32)
    sub = lax.broadcasted_iota(jnp.int32, (width, slots), 0)
    for g in range(groups):
        choose = jnp.where(sub == sticks[g], 1.0, 0.0).astype(BF16)
        dense += dot(choose, spread[g])
    dense = dense.astype(BF16)

    loads[2].wait()
    columns = dot(dense, tz[0]) + dot(dense, tz[1])
    col_hi, col_lo = split(columns)
    colbuf[0, :width] = col_hi[:, :plane_pad]
    colbuf[0, width:] = col_hi[:, plane_pad:]
    colbuf[1, :width] = col_lo[:, :plane_pad]
    colbuf[1, width:] = col_lo[:, plane_pad:]
    loads[3].wait()
    field = dot(tx[0], colbuf[0]) + dot(tx[0], colbuf[1]) + dot(tx[1], colbuf[0])
    product = jnp.concatenate([field[:coarse] * weight, field[coarse:] * weight], axis=0)
    pro_hi, pro_lo = split(product)
    loads[4].wait()
    back = dot(ty[0], pro_hi) + dot(ty[0], pro_lo) + dot(ty[1], pro_hi)
    back = jnp.concatenate([back[:width], back[width:]], axis=1)
    back_hi, back_lo = split(back)
    spectra = dot_nt(back_hi, tz[0]) + dot_nt(back_hi, tz[1]) + dot_nt(back_lo, tz[0])
    spectra = spectra * (1.0 / float(points * coarse))
    spec_hi, spec_lo = split(spectra)

    eye = lax.broadcasted_iota(jnp.int32, (slots, slots), 0) == lax.broadcasted_iota(
        jnp.int32, (slots, slots), 1
    )

    def stick_column(g):
        row = sticks[0]
        for other in range(1, groups):
            row = jnp.where(g == other, sticks[other], row)
        row = row.astype(F32)
        return jnp.sum(jnp.where(eye, row, 0.0), axis=1, keepdims=True)

    lane_f = lane.astype(F32)
    p_copies = []
    for k in range(1, groups + 1):
        target = lax.rem(ga + k, groups)
        stick = stick_column(target)
        choose = jnp.where(stick == lane_f, 1.0, 0.0).astype(BF16)
        mine = dot(choose, spec_hi) + dot(choose, spec_lo)
        if k < groups:
            part[k - 1] = mine
            copy = pltpu.make_async_remote_copy(
                src_ref=part.at[k - 1],
                dst_ref=got.at[k - 1],
                send_sem=p_send.at[k - 1],
                recv_sem=p_recv.at[k - 1],
                device_id=(band, target),
                device_id_type=MESH,
            )
            copy.start()
            p_copies.append(copy)

    present = own >= 0
    gx = stick - float(radius - 1)
    gz = (own - (radius - 1)).astype(F32)
    kinetic = (gx * gx + gz * gz) * (1.0 / float(radius * radius))
    own_index = jnp.maximum(own, 0)

    gather[0] = orb_ref[:, 0]
    m_re = jnp.where(present, re, 0.0)
    m_im = jnp.where(present, im, 0.0)

    def add_products(first, right_re, right_im, fresh):
        @pl.loop(0, half + 1)
        def _(k):
            if fresh:
                @pl.when(k > 0)
                def _():
                    gather_copy(k).wait()

            b = lax.rem(band - k + bands, bands)
            left_re = gather[k, 0].astype(F32)
            left_im = gather[k, 1].astype(F32)
            real = left_re * right_re + left_im * right_im
            imag = left_re * right_im - left_im * right_re
            sums[pl.ds(first * bands + b, 1), :] = jnp.sum(real, axis=0, keepdims=True)
            sums[pl.ds((first + 1) * bands + b, 1), :] = jnp.sum(imag, axis=0, keepdims=True)

    add_products(0, m_re, m_im, True)

    for copy in p_copies:
        copy.wait()
    for k in range(1, groups):
        mine += got[k - 1]
    a_re = take_lanes(mine[:, :width], own_index)
    a_im = take_lanes(mine[:, width:], own_index)
    h_re = jnp.where(present, kinetic * re + a_re, 0.0).astype(BF16)
    h_im = jnp.where(present, kinetic * im + a_im, 0.0).astype(BF16)
    out_ref[0, 0] = h_re
    out_ref[1, 0] = h_im
    add_products(2, h_re.astype(F32), h_im.astype(F32), False)

    ones = jnp.full((8, width), 1.0 / float(4 * radius * radius), F32)
    row = lax.dot_general(
        ones, sums[...], NT, preferred_element_type=F32, precision=lax.Precision.HIGHEST
    )
    message[...] = row[:1]
    inbox[pl.ds(me, 1), 0, :] = row[:1]

    @pl.loop(1, total)
    def _(k):
        pltpu.make_async_remote_copy(
            src_ref=message,
            dst_ref=inbox.at[me],
            send_sem=m_send,
            recv_sem=m_recv,
            device_id=where_is(lax.rem(me + k, total)),
            device_id_type=MESH,
        ).start()

    everyone = inbox.at[pl.ds(0, total - 1)]
    pltpu.make_async_copy(everyone, everyone, m_recv).wait()
    pltpu.make_async_copy(everyone, everyone, m_send).wait()

    rows = inbox[0:bands, 0, :]
    for g in range(1, groups):
        rows += inbox[g * bands : (g + 1) * bands, 0, :]
    unit = (
        lax.broadcasted_iota(jnp.int32, (msg_width, msg_width), 0)
        == lax.broadcasted_iota(jnp.int32, (msg_width, msg_width), 1)
    ).astype(F32)
    turned = lax.dot_general(
        unit, rows, NT, preferred_element_type=F32, precision=lax.Precision.HIGHEST
    )
    place_i = lax.broadcasted_iota(jnp.int32, (bands, bands), 0)
    place_j = lax.broadcasted_iota(jnp.int32, (bands, bands), 1)
    direct = lax.rem(place_j - place_i + bands, bands) <= half

    def assemble(c, sign):
        part_of = slice(c * bands, (c + 1) * bands)
        return jnp.where(direct, turned[part_of], sign * rows[:, part_of])

    corr_ref[0] = assemble(0, 1.0)
    corr_ref[1] = assemble(1, -1.0)
    red_ref[0] = assemble(2, 1.0)
    red_ref[1] = assemble(3, -1.0)


def body(bands, groups, orbitals, potential, slot_sticks, stick_entries):
    points = potential.shape[1]
    planes = potential.shape[0]
    width = stick_entries.shape[1]
    radius = width // 2
    slots = orbitals.shape[2]
    plane_pad = -(-planes // 128) * 128
    coarse = 2 * width
    sum_rows = -(-4 * bands // 128) * 128
    tz, tx, ty, tr = tables(points, width, radius, groups, planes, plane_pad, coarse)
    vmem = pl.BlockSpec(memory_space=pltpu.VMEM)
    hbm = pl.BlockSpec(memory_space=pltpu.HBM)
    total = bands * groups
    dma = pltpu.SemaphoreType.DMA
    return pl.pallas_call(
        functools.partial(kernel, bands, groups, points, radius),
        out_shape=(
            jax.ShapeDtypeStruct(orbitals.shape, BF16),
            jax.ShapeDtypeStruct((2, bands, bands), F32),
            jax.ShapeDtypeStruct((2, bands, bands), F32),
        ),
        in_specs=[hbm] * 8,
        out_specs=(vmem, vmem, vmem),
        scratch_shapes=[
            pltpu.VMEM(orbitals.shape, BF16),
            pltpu.VMEM(slot_sticks.shape, jnp.int32),
            pltpu.VMEM((slots, width), jnp.int32),
            pltpu.VMEM(tz.shape[1:], BF16),
            pltpu.VMEM(tx.shape, BF16),
            pltpu.VMEM(ty.shape, BF16),
            pltpu.VMEM(tr.shape, BF16),
            pltpu.VMEM((plane_pad, points), F32),
            pltpu.VMEM((groups, slots, 2 * width), BF16),
            pltpu.VMEM((2, 2 * width, plane_pad), BF16),
            pltpu.VMEM((groups - 1, slots, 2 * width), F32),
            pltpu.VMEM((groups - 1, slots, 2 * width), F32),
            pltpu.VMEM((bands // 2 + 1, 2, slots, width), BF16),
            pltpu.VMEM((sum_rows, width), F32),
            pltpu.VMEM((1, sum_rows), F32),
            pltpu.VMEM((total, 1, sum_rows), F32),
            dma((8,)),
            dma((groups - 1,)),
            dma((groups - 1,)),
            dma((groups - 1,)),
            dma((groups - 1,)),
            dma((bands // 2 + 1,)),
            dma((bands // 2 + 1,)),
            dma,
            dma,
        ],
        compiler_params=pltpu.CompilerParams(
            collective_id=0, has_side_effects=True, vmem_limit_bytes=67043328 - 81920
        ),
    )(orbitals, slot_sticks, stick_entries, potential, tz, tx, ty, tr)


def solution(mesh):
    bands = mesh.shape["band"]
    groups = mesh.shape["ga"]
    return jax.shard_map(
        functools.partial(body, bands, groups),
        mesh=mesh,
        in_specs=(P(None, "band", "ga", None), P("ga", None), P(), P()),
        out_specs=(P(None, "band", "ga", None), P(), P()),
        check_vma=False,
    )
```

```python
import functools

import jax
import jax.numpy as jnp
import numpy as np
from jax import lax
from jax.experimental import pallas as pl
from jax.experimental.pallas import tpu as pltpu
from jax.sharding import PartitionSpec as P

MESH = pl.DeviceIdType.MESH
NT = (((1,), (1,)), ((), ()))
BF16 = jnp.bfloat16
F32 = jnp.float32


def split_np(table):
    high = table.astype(np.float32).astype(BF16)
    low = (table - high.astype(np.float64)).astype(np.float32).astype(BF16)
    return np.stack([high, low])


def tables(points, width, radius, groups, planes, plane_pad, coarse):
    freq = np.arange(width) - radius + 1
    used = (np.arange(width) < width - 1).astype(np.float64)
    z_tabs = []
    for group in range(groups):
        z = np.arange(planes) + group * planes
        angle = 2.0 * np.pi * ((freq[:, None] * z[None, :]) % points) / points
        cos = np.zeros((width, plane_pad))
        sin = np.zeros((width, plane_pad))
        cos[:, :planes] = np.cos(angle) * used[:, None]
        sin[:, :planes] = np.sin(angle) * used[:, None]
        z_tabs.append(split_np(np.block([[cos, sin], [-sin, cos]])))
    x = np.arange(coarse)
    angle = 2.0 * np.pi * ((freq[None, :] * x[:, None]) % coarse) / coarse
    cos = np.cos(angle) * used[None, :]
    sin = np.sin(angle) * used[None, :]
    forward = np.block([[cos, -sin], [sin, cos]])
    limit = 2 * (radius - 1)
    offset = (x[:, None] * points - np.arange(points)[None, :] * coarse) % (coarse * points)
    base = 2.0 * np.pi * offset / (coarse * points)
    resample = np.ones((coarse, points))
    for g in range(1, limit + 1):
        resample += 2.0 * np.cos(g * base)
    resample /= points
    return (
        np.stack(z_tabs),
        split_np(forward),
        split_np(forward.T.copy()),
        split_np(resample),
    )


def split(value):
    high = value.astype(BF16)
    low = (value - high.astype(F32)).astype(BF16)
    return high, low


def dot(a, b):
    return jnp.dot(a, b, preferred_element_type=F32)


def dot_nt(a, b):
    return lax.dot_general(a, b, NT, preferred_element_type=F32)


def take_lanes(value, index):
    return jnp.take_along_axis(value, index, axis=1, mode="promise_in_bounds")


def kernel(
    bands,
    groups,
    points,
    radius,
    orb_hbm,
    slots_hbm,
    entries_hbm,
    pot_hbm,
    tz_hbm,
    tx_hbm,
    ty_hbm,
    tr_hbm,
    out_ref,
    corr_ref,
    red_ref,
    orb_ref,
    slots_ref,
    entries_ref,
    tz,
    tx,
    ty,
    tr,
    pot,
    spread,
    colbuf,
    part,
    got,
    gather,
    sums,
    message,
    inbox,
    load_sem,
    s_send,
    s_recv,
    p_send,
    p_recv,
    g_send,
    g_recv,
    m_send,
    m_recv,
):
    band = lax.axis_index("band")
    ga = lax.axis_index("ga")
    total = bands * groups
    half = bands // 2
    me = ga * bands + band
    slots = orb_hbm.shape[2]
    width = orb_hbm.shape[3]
    planes = pot_hbm.shape[0]
    plane_pad = pot.shape[0]
    coarse = ty.shape[2] // 2
    msg_width = message.shape[1]

    def where_is(index):
        return (lax.rem(index, bands), lax.div(index, bands))

    barrier = pltpu.get_barrier_semaphore()

    @pl.loop(1, total)
    def _(k):
        pl.semaphore_signal(
            barrier, inc=1, device_id=where_is(lax.rem(me + k, total)), device_id_type=MESH
        )

    first = [
        pltpu.make_async_copy(
            entries_hbm.at[pl.ds(pl.multiple_of(ga * slots, 8), slots)], entries_ref, load_sem.at[5]
        ),
        pltpu.make_async_copy(orb_hbm, orb_ref, load_sem.at[6]),
        pltpu.make_async_copy(slots_hbm, slots_ref, load_sem.at[7]),
    ]
    for load in first:
        load.start()
    loads = [
        pltpu.make_async_copy(pot_hbm, pot.at[pl.ds(0, planes)], load_sem.at[0]),
        pltpu.make_async_copy(tr_hbm, tr, load_sem.at[1]),
        pltpu.make_async_copy(tz_hbm.at[ga], tz, load_sem.at[2]),
        pltpu.make_async_copy(tx_hbm, tx, load_sem.at[3]),
        pltpu.make_async_copy(ty_hbm, ty, load_sem.at[4]),
    ]
    for load in loads:
        load.start()
    if plane_pad > planes:
        pot[pl.ds(planes, plane_pad - planes), :] = jnp.zeros(
            (plane_pad - planes, pot.shape[1]), F32
        )

    sums[...] = jnp.zeros_like(sums)

    for load in first:
        load.wait()
    own = entries_ref[...]
    all_sticks = slots_ref[...].reshape(1, groups * slots)
    sticks = [all_sticks[:, g * slots : (g + 1) * slots] for g in range(groups)]
    lane = lax.broadcasted_iota(jnp.int32, (slots, width), 1)
    inverse = jnp.full((slots, width), -1, jnp.int32)
    for k in range(width):
        inverse = jnp.where(own[:, k : k + 1] == lane, k, inverse)
    re = orb_ref[0, 0].astype(F32)
    im = orb_ref[1, 0].astype(F32)
    filled = inverse >= 0
    index = jnp.maximum(inverse, 0)
    spread[ga, :, :width] = jnp.where(filled, take_lanes(re, index), 0.0).astype(BF16)
    spread[ga, :, width:] = jnp.where(filled, take_lanes(im, index), 0.0).astype(BF16)

    pl.semaphore_wait(barrier, total - 1)

    s_copies = []
    for k in range(1, groups):
        copy = pltpu.make_async_remote_copy(
            src_ref=spread.at[ga],
            dst_ref=spread.at[ga],
            send_sem=s_send.at[k - 1],
            recv_sem=s_recv.at[k - 1],
            device_id=(band, lax.rem(ga + k, groups)),
            device_id_type=MESH,
        )
        copy.start()
        s_copies.append(copy)

    def gather_copy(k):
        return pltpu.make_async_remote_copy(
            src_ref=orb_hbm.at[:, 0],
            dst_ref=gather.at[k],
            send_sem=g_send.at[k],
            recv_sem=g_recv.at[k],
            device_id=(lax.rem(band + k, bands), ga),
            device_id_type=MESH,
        )

    @pl.loop(1, half + 1)
    def _(k):
        gather_copy(k).start()

    loads[0].wait()
    loads[1].wait()
    pot_hi, pot_lo = split(pot[...])
    weight = dot_nt(tr[0], pot_hi) + dot_nt(tr[0], pot_lo) + dot_nt(tr[1], pot_hi)

    for copy in s_copies:
        copy.wait()
    dense = jnp.zeros((width, 2 * width), F32)
    sub = lax.broadcasted_iota(jnp.int32, (width, slots), 0)
    for g in range(groups):
        choose = jnp.where(sub == sticks[g], 1.0, 0.0).astype(BF16)
        dense += dot(choose, spread[g])
    dense = dense.astype(BF16)

    loads[2].wait()
    columns = dot(dense, tz[0]) + dot(dense, tz[1])
    col_hi, col_lo = split(columns)
    colbuf[0, :width] = col_hi[:, :plane_pad]
    colbuf[0, width:] = col_hi[:, plane_pad:]
    colbuf[1, :width] = col_lo[:, :plane_pad]
    colbuf[1, width:] = col_lo[:, plane_pad:]
    loads[3].wait()
    field = dot(tx[0], colbuf[0]) + dot(tx[0], colbuf[1]) + dot(tx[1], colbuf[0])
    product = jnp.concatenate([field[:coarse] * weight, field[coarse:] * weight], axis=0)
    pro_hi, pro_lo = split(product)
    loads[4].wait()
    back = dot(ty[0], pro_hi) + dot(ty[0], pro_lo) + dot(ty[1], pro_hi)
    back = jnp.concatenate([back[:width], back[width:]], axis=1)
    back_hi, back_lo = split(back)
    spectra = dot_nt(back_hi, tz[0]) + dot_nt(back_hi, tz[1]) + dot_nt(back_lo, tz[0])
    spectra = spectra * (1.0 / float(points * coarse))
    spec_hi, spec_lo = split(spectra)

    eye = lax.broadcasted_iota(jnp.int32, (slots, slots), 0) == lax.broadcasted_iota(
        jnp.int32, (slots, slots), 1
    )

    def stick_column(g):
        row = sticks[0]
        for other in range(1, groups):
            row = jnp.where(g == other, sticks[other], row)
        row = row.astype(F32)
        return jnp.sum(jnp.where(eye, row, 0.0), axis=1, keepdims=True)

    lane_f = lane.astype(F32)
    p_copies = []
    for k in range(1, groups + 1):
        target = lax.rem(ga + k, groups)
        stick = stick_column(target)
        choose = jnp.where(stick == lane_f, 1.0, 0.0).astype(BF16)
        mine = dot(choose, spec_hi) + dot(choose, spec_lo)
        if k < groups:
            part[k - 1] = mine
            copy = pltpu.make_async_remote_copy(
                src_ref=part.at[k - 1],
                dst_ref=got.at[k - 1],
                send_sem=p_send.at[k - 1],
                recv_sem=p_recv.at[k - 1],
                device_id=(band, target),
                device_id_type=MESH,
            )
            copy.start()
            p_copies.append(copy)

    present = own >= 0
    gx = stick - float(radius - 1)
    gz = (own - (radius - 1)).astype(F32)
    kinetic = (gx * gx + gz * gz) * (1.0 / float(radius * radius))
    own_index = jnp.maximum(own, 0)

    gather[0] = orb_ref[:, 0]
    m_re = jnp.where(present, re, 0.0)
    m_im = jnp.where(present, im, 0.0)

    def add_products(first, right_re, right_im, fresh):
        @pl.loop(0, half + 1)
        def _(k):
            if fresh:
                @pl.when(k > 0)
                def _():
                    gather_copy(k).wait()

            b = lax.rem(band - k + bands, bands)
            left_re = gather[k, 0].astype(F32)
            left_im = gather[k, 1].astype(F32)
            real = left_re * right_re + left_im * right_im
            imag = left_re * right_im - left_im * right_re
            sums[pl.ds(first * bands + b, 1), :] = jnp.sum(real, axis=0, keepdims=True)
            sums[pl.ds((first + 1) * bands + b, 1), :] = jnp.sum(imag, axis=0, keepdims=True)

    add_products(0, m_re, m_im, True)

    for copy in p_copies:
        copy.wait()
    for k in range(1, groups):
        mine += got[k - 1]
    a_re = take_lanes(mine[:, :width], own_index)
    a_im = take_lanes(mine[:, width:], own_index)
    h_re = jnp.where(present, kinetic * re + a_re, 0.0).astype(BF16)
    h_im = jnp.where(present, kinetic * im + a_im, 0.0).astype(BF16)
    out_ref[0, 0] = h_re
    out_ref[1, 0] = h_im
    add_products(2, h_re.astype(F32), h_im.astype(F32), False)

    ones = jnp.full((8, width), 1.0 / float(4 * radius * radius), F32)
    row = lax.dot_general(
        ones, sums[...], NT, preferred_element_type=F32, precision=lax.Precision.HIGHEST
    )
    message[...] = row[:1]
    inbox[pl.ds(me, 1), 0, :] = row[:1]

    @pl.loop(1, total)
    def _(k):
        pltpu.make_async_remote_copy(
            src_ref=message,
            dst_ref=inbox.at[me],
            send_sem=m_send,
            recv_sem=m_recv,
            device_id=where_is(lax.rem(me + k, total)),
            device_id_type=MESH,
        ).start()

    everyone = inbox.at[pl.ds(0, total - 1)]
    pltpu.make_async_copy(everyone, everyone, m_recv).wait()
    pltpu.make_async_copy(everyone, everyone, m_send).wait()

    rows = inbox[0:bands, 0, :]
    for g in range(1, groups):
        rows += inbox[g * bands : (g + 1) * bands, 0, :]
    unit = (
        lax.broadcasted_iota(jnp.int32, (msg_width, msg_width), 0)
        == lax.broadcasted_iota(jnp.int32, (msg_width, msg_width), 1)
    ).astype(F32)
    turned = lax.dot_general(
        unit, rows, NT, preferred_element_type=F32, precision=lax.Precision.HIGHEST
    )
    place_i = lax.broadcasted_iota(jnp.int32, (bands, bands), 0)
    place_j = lax.broadcasted_iota(jnp.int32, (bands, bands), 1)
    direct = lax.rem(place_j - place_i + bands, bands) <= half

    def assemble(c, sign):
        part_of = slice(c * bands, (c + 1) * bands)
        return jnp.where(direct, turned[part_of], sign * rows[:, part_of])

    corr_ref[0] = assemble(0, 1.0)
    corr_ref[1] = assemble(1, -1.0)
    red_ref[0] = assemble(2, 1.0)
    red_ref[1] = assemble(3, -1.0)


def body(bands, groups, orbitals, potential, slot_sticks, stick_entries):
    points = potential.shape[1]
    planes = potential.shape[0]
    width = stick_entries.shape[1]
    radius = width // 2
    slots = orbitals.shape[2]
    plane_pad = -(-planes // 128) * 128
    coarse = 2 * width
    sum_rows = -(-4 * bands // 128) * 128
    tz, tx, ty, tr = tables(points, width, radius, groups, planes, plane_pad, coarse)
    vmem = pl.BlockSpec(memory_space=pltpu.VMEM)
    hbm = pl.BlockSpec(memory_space=pltpu.HBM)
    total = bands * groups
    dma = pltpu.SemaphoreType.DMA
    return pl.pallas_call(
        functools.partial(kernel, bands, groups, points, radius),
        out_shape=(
            pltpu.VMEM(orbitals.shape, BF16),
            pltpu.VMEM((2, bands, bands), F32),
            pltpu.VMEM((2, bands, bands), F32),
        ),
        in_specs=[hbm] * 8,
        out_specs=(vmem, vmem, vmem),
        scratch_shapes=[
            pltpu.VMEM(orbitals.shape, BF16),
            pltpu.VMEM(slot_sticks.shape, jnp.int32),
            pltpu.VMEM((slots, width), jnp.int32),
            pltpu.VMEM(tz.shape[1:], BF16),
            pltpu.VMEM(tx.shape, BF16),
            pltpu.VMEM(ty.shape, BF16),
            pltpu.VMEM(tr.shape, BF16),
            pltpu.VMEM((plane_pad, points), F32),
            pltpu.VMEM((groups, slots, 2 * width), BF16),
            pltpu.VMEM((2, 2 * width, plane_pad), BF16),
            pltpu.VMEM((groups - 1, slots, 2 * width), F32),
            pltpu.VMEM((groups - 1, slots, 2 * width), F32),
            pltpu.VMEM((bands // 2 + 1, 2, slots, width), BF16),
            pltpu.VMEM((sum_rows, width), F32),
            pltpu.VMEM((1, sum_rows), F32),
            pltpu.VMEM((total, 1, sum_rows), F32),
            dma((8,)),
            dma((groups - 1,)),
            dma((groups - 1,)),
            dma((groups - 1,)),
            dma((groups - 1,)),
            dma((bands // 2 + 1,)),
            dma((bands // 2 + 1,)),
            dma,
            dma,
        ],
        compiler_params=pltpu.CompilerParams(
            collective_id=0, has_side_effects=True, vmem_limit_bytes=60000000
        ),
    )(orbitals, slot_sticks, stick_entries, potential, tz, tx, ty, tr)


def solution(mesh):
    bands = mesh.shape["band"]
    groups = mesh.shape["ga"]
    return jax.shard_map(
        functools.partial(body, bands, groups),
        mesh=mesh,
        in_specs=(P(None, "band", "ga", None), P("ga", None), P(), P()),
        out_specs=(P(None, "band", "ga", None), P(), P()),
        check_vma=False,
    )
```
